32 devices in a mesh: depth: 4 (over y, x), screen: 8 (over z, core).
Axes of the slice: x: 2, y: 2, z: 4, core: 2. Of those that a mesh axis runs over, the one named last changes fastest.
Arguments:
- voxel_bins: int32 [32, 256, 2048], P('depth', None, 'screen'), may hold values from 0 to 255
- colors: bfloat16 [3, 256], replicated, may hold values from 0 to 2
- opacity: bfloat16 [256], replicated, may hold values from 0 to 1
- slab_order: int32 [8, 4], replicated, may hold values from 0 to 3, each once within a row
Outputs:
- image: float32 [4, 256, 2048], P(None, ('depth', 'screen'))
The draws below stay inside these ranges and needn't reach their ends.
Inputs may be any that keep to these rules, and one draw needn't show every extreme that they name: `slab_order`: every row is a permutation of 0 to 3.
All inputs are finite; a program needn't handle non-finite values.
Results may differ from the reference program's by a relative error of at most 0.0003.
Values sent between devices are 32-bit elements; how exact they have to be, the bound alone decides.
A program may use at most 64 MiB of HBM per device.

```python
import jax
import jax.numpy as jnp
from jax import lax

NBINS = 256
IMG_H = 256
SAMPLES = 32
IMG_W = 2048
DEPTHS = 4
TILES = 8


def place_ends(result, own_key, least, largest):
    extent = result.shape
    index_at = [jax.random.randint(jax.random.fold_in(own_key, axis), (), 0, extent[axis]) for axis in range(len(extent))]
    result = result.at[tuple(index_at)].set(least)
    longest = extent.index(max(extent))
    index_at[longest] = (index_at[longest] + 1) % extent[longest]
    return result.at[tuple(index_at)].set(largest)


def setup_inputs(seed: int = 0) -> dict:
    arg_keys = jax.random.split(jax.random.key(seed), 5)
    voxel_bins = place_ends(jax.random.randint(arg_keys[0], (SAMPLES, IMG_H, IMG_W), 0, NBINS), jax.random.fold_in(arg_keys[0], 1), 0, NBINS - 1).astype(jnp.int32)
    colors = jnp.clip(jax.random.uniform(arg_keys[1], (3, NBINS), jnp.float32, 0.0, 2.0), 0.0, 2.0).astype(jnp.bfloat16)
    opacity = jnp.clip(jax.random.uniform(arg_keys[2], (NBINS,), jnp.float32, 0.0, 1.0), 0.0, 1.0).astype(jnp.bfloat16)
    slab_order = jax.vmap(lambda own: jax.random.permutation(own, DEPTHS))(jax.random.split(arg_keys[3], TILES)).reshape((TILES, DEPTHS)).astype(jnp.int32)
    return dict(voxel_bins=voxel_bins, colors=colors, opacity=opacity, slab_order=slab_order)


def reference(voxel_bins, colors, opacity, slab_order):
    table = jnp.concatenate([colors, opacity[None]], axis=0).astype(jnp.float32)
    sample_total = voxel_bins.shape[0]
    slab_count = slab_order.shape[1]
    tile_count = slab_order.shape[0]
    row_count = voxel_bins.shape[1]
    col_count = voxel_bins.shape[2]
    extinct_rate = 3.0 / sample_total
    slabs = voxel_bins.reshape(slab_count, sample_total // slab_count, row_count, col_count)

    def march(slab):
        def advance(carried, layer):
            passed, color_sum = carried
            values = jnp.take(table, layer, axis=1)
            density = values[3]
            weight = (1.0 - jnp.exp(-extinct_rate * density)) * jnp.exp(-extinct_rate * passed)
            return (passed + density, color_sum + weight[None] * values[:3]), None

        start = (jnp.zeros((row_count, col_count), jnp.float32), jnp.zeros((3, row_count, col_count), jnp.float32))
        (passed, color_sum), ignored = lax.scan(advance, start, slab)
        final_alpha = 1.0 - jnp.exp(-extinct_rate * passed)
        return jnp.concatenate([color_sum, final_alpha[None]], axis=0)

    partials = lax.map(march, slabs)
    pieces = partials.reshape(slab_count, 4, row_count, tile_count, col_count // tile_count)
    acc_color = jnp.zeros((3, row_count, tile_count, col_count // tile_count), jnp.float32)
    acc_alpha = jnp.zeros((row_count, tile_count, col_count // tile_count), jnp.float32)
    for place in range(slab_count):
        select = (slab_order == place).astype(jnp.float32)
        picked = jnp.einsum("ti,icrtw->crtw", select, pieces, precision=lax.Precision.HIGHEST)
        acc_color = acc_color + (1.0 - acc_alpha)[None] * picked[:3]
        acc_alpha = acc_alpha + (1.0 - acc_alpha) * picked[3]
    merged = jnp.concatenate([acc_color, acc_alpha[None]], axis=0)
    return merged.reshape(4, row_count, col_count)
```

```python
import functools

import jax
import jax.numpy as jnp
from jax import lax
from jax.experimental import pallas as pl
from jax.experimental.pallas import tpu as pltpu
from jax.sharding import PartitionSpec as P

extinction = 3.0
lanes = 128
HEAD, LAG = 2, 4
MESH = pl.DeviceIdType.MESH


def flip(index, mask, count):
    result = index
    bit = 1
    while bit < count:
        if isinstance(mask, int):
            if mask & bit:
                result = result + bit * (1 - 2 * lax.rem(lax.div(index, bit), 2))
        else:
            mine = lax.rem(lax.div(index, bit), 2)
            other = lax.rem(lax.div(mask, bit), 2)
            result = result + bit * other * (1 - 2 * mine)
        bit *= 2
    return result


def kernel(
    sizes,
    order_ref,
    bins_hbm,
    colors_ref,
    opacity_ref,
    out_ref,
    bins,
    sent,
    own,
    arrived,
    merged,
    bins_sem,
    send_sem,
    recv_sem,
    row_send_sem,
    row_recv_sem,
    pass_sem,
    passed,
    pass_send_sem,
    pass_recv_sem,
):
    depth_count, tile_count, samples, unit_rows, units, owners, rows_each, cols, rate = sizes
    depth = lax.axis_index("depth")
    tile = lax.axis_index("screen")
    own_unit = lax.div(tile, owners)
    own_place = lax.rem(tile, owners)
    steps = list(range(units - 1, -1, -1))
    crossing = [2] if owners == 1 and units > 3 else []
    peers = [depth_count - 1] + list(range(1, depth_count - 1)) + [0]

    barrier = pltpu.get_barrier_semaphore()
    near = [mask for mask in peers if mask and not mask & (mask - 1)]
    far = [mask for mask in peers if mask & (mask - 1)]
    below = tile >= 2
    above = tile + 2 < tile_count
    beside = 1 + below.astype(jnp.int32) + above.astype(jnp.int32)

    def greet(sem):
        def tell(there):
            pl.semaphore_signal(sem, inc=1, device_id=(depth, there), device_id_type=MESH)

        tell(flip(tile, 1, tile_count))

        @pl.when(below)
        def _():
            tell(tile - 2)

        @pl.when(above)
        def _():
            tell(tile + 2)

    rounds = tile_count // 2 - 1

    def widen(first, last):
        for n in range(first, min(last, rounds)):
            pl.semaphore_wait(pass_sem.at[n], beside)
            if n + 1 < rounds:
                greet(pass_sem.at[n + 1])

    for mask in far + near:
        peer = flip(depth, mask, depth_count)
        pl.semaphore_signal(barrier, inc=1, device_id=(peer, tile), device_id_type=MESH)
    greet(barrier)

    def fetch(step, mask):
        row = (flip(depth, mask, depth_count) * units + flip(own_unit, step, units)) * unit_rows
        row = pl.multiple_of(row, unit_rows)
        return pltpu.make_async_copy(
            bins_hbm.at[:, pl.ds(row, unit_rows), :],
            bins.at[step, mask],
            bins_sem.at[step, mask],
        )

    for mask in far + near:
        fetch(steps[0], mask).start()

    def fetch_rest():
        for step in steps[1:2] + crossing + [k for k in steps[2:] if k not in crossing]:
            for mask in far + near:
                fetch(step, mask).start()
        for step in crossing + [k for k in steps if k not in crossing]:
            fetch(step, 0).start()


    density = opacity_ref[...].astype(jnp.float32).reshape(1, -1)
    weight = 1.0 - jnp.exp(-rate * density)
    shades = weight * colors_ref[...].astype(jnp.float32)
    table = [shades[c : c + 1] for c in range(3)] + [weight]
    bin_count = weight.shape[1]
    parts = [
        [jnp.broadcast_to(row[:, at : at + lanes], (8, lanes)) for at in range(0, bin_count, lanes)]
        for row in table
    ]

    def march(step, mask, target):
        for row in range(0, unit_rows, 8):
            for col in range(0, cols, lanes):
                clear = None
                total = None
                for j in range(samples):
                    index = bins[step, mask, j, row : row + 8, col : col + lanes]
                    low = lax.rem(index, lanes) if lanes & (lanes - 1) else index & (lanes - 1)
                    values = []
                    for part in parts:
                        value = jnp.take_along_axis(part[0], low, axis=1, mode="promise_in_bounds")
                        for n in range(1, len(part)):
                            other = jnp.take_along_axis(
                                part[n], low, axis=1, mode="promise_in_bounds"
                            )
                            value = jnp.where(index >= n * lanes, other, value)
                        values.append(value)
                    if total is None:
                        total = values
                        clear = 1.0 - values[3]
                    else:
                        seen = clear * values[3]
                        total = [t + clear * v for t, v in zip(total[:3], values[:3])] + [
                            total[3] + seen
                        ]
                        clear = clear - seen
                for c in range(4):
                    target[c, row : row + 8, col : col + lanes] = total[c]

    def send(step, mask):
        return pltpu.make_async_remote_copy(
            src_ref=sent.at[step, mask - 1],
            dst_ref=arrived.at[step, mask - 1],
            send_sem=send_sem.at[step, mask - 1],
            recv_sem=recv_sem.at[step, mask - 1],
            device_id=(flip(depth, mask, depth_count), tile),
            device_id_type=MESH,
        )

    def send_row(step, low):
        mask = step * owners + low
        place = flip(own_place, low, owners)
        there = pl.ds(pl.multiple_of(tile * cols, lanes), cols)
        return pltpu.make_async_remote_copy(
            src_ref=merged.at[step, place],
            dst_ref=out_ref.at[:, :, there],
            send_sem=row_send_sem.at[mask],
            recv_sem=row_recv_sem.at[mask],
            device_id=(depth, flip(tile, mask, tile_count)),
            device_id_type=MESH,
        )

    def take_row(mask):
        here = pl.ds(pl.multiple_of(flip(tile, mask, tile_count) * cols, lanes), cols)
        return pltpu.make_async_remote_copy(
            src_ref=merged.at[0, 0],
            dst_ref=out_ref.at[:, :, here],
            send_sem=row_send_sem.at[mask],
            recv_sem=row_recv_sem.at[mask],
            device_id=(depth, flip(tile, mask, tile_count)),
            device_id_type=MESH,
        )

    def carry_over(step, mask):
        return pltpu.make_async_remote_copy(
            src_ref=sent.at[step, mask - 1] if mask else own.at[step],
            dst_ref=passed.at[mask],
            send_sem=pass_send_sem.at[mask],
            recv_sem=pass_recv_sem.at[mask],
            device_id=(depth, flip(tile, step, tile_count)),
            device_id_type=MESH,
        )

    def hand_on(step, mask):
        return pltpu.make_async_remote_copy(
            src_ref=passed.at[mask],
            dst_ref=arrived.at[step, mask - 1],
            send_sem=send_sem.at[step, mask - 1],
            recv_sem=recv_sem.at[step, mask - 1],
            device_id=(flip(depth, mask, depth_count), tile),
            device_id_type=MESH,
        )

    def cross():
        for step in crossing:
            for mask in far + near + [0]:
                fetch(step, mask).wait()
                march(step, mask, sent.at[step, mask - 1] if mask else own.at[step])
                carry_over(step, mask).start()

    def feed(n):
        step = units - 1 - n

        def plain():
            for mask in far + near:
                fetch(step, mask).wait()
                march(step, mask, sent.at[step, mask - 1])
                send(step, mask).start()

        if not crossing:
            plain()
            return
        pl.when(step != crossing[0])(plain)

        @pl.when(step == crossing[0])
        def _():
            for mask in far + near:
                carry_over(crossing[0], mask).wait_recv()
                hand_on(crossing[0], mask).start()

    def fronts(of_tile):
        place_of = [
            order_ref[flip(depth, mask, depth_count), of_tile] for mask in range(depth_count)
        ]
        return [
            [jnp.where(place_of[j] < place_of[i], 1.0, 0.0) for j in range(depth_count)]
            for i in range(depth_count)
        ]

    def merge(pieces_at, ahead, put):
        for row in range(0, unit_rows, 8):
            for col in range(0, cols, lanes):
                pieces = pieces_at(row, col)
                total = None
                for i in range(depth_count):
                    front = None
                    for j in range(depth_count):
                        if j != i:
                            clear = 1.0 - ahead[i][j] * pieces[j][3]
                            front = clear if front is None else front * clear
                    lit = [pieces[i][c] if front is None else pieces[i][c] * front for c in range(4)]
                    total = lit if total is None else [t + v for t, v in zip(total, lit)]
                put(row, col, total)

    ahead = fronts(tile)

    def blend(n):
        step = units - 1 - n

        def plain():
            fetch(step, 0).wait()
            march(step, 0, own.at[step])
            for mask in far + near:
                send(step, mask).wait_recv()

            def pieces_at(row, col):
                window = (slice(None), slice(row, row + 8), slice(col, col + lanes))
                return [
                    own[(step,) + window] if mask == 0 else arrived[(step, mask - 1) + window]
                    for mask in range(depth_count)
                ]

            def put(row, col, total):
                for c in range(4):
                    if owners == 1:
                        merged[step, 0, c, row : row + 8, col : col + lanes] = total[c]
                    else:
                        for place in range(owners):
                            merged[step, place, c, :, col : col + lanes] = total[c][
                                place * rows_each : (place + 1) * rows_each
                            ]

            merge(pieces_at, ahead, put)
            for low in range(owners - 1, 0, -1):
                send_row(step, low).start()

            @pl.when(step > 0)
            def _():
                send_row(step, 0).start()

        if not crossing:
            plain()
            return
        pl.when(step != crossing[0])(plain)

        @pl.when(step == crossing[0])
        def _():
            there = flip(tile, crossing[0], tile_count)
            carry_over(crossing[0], 0).wait_recv()
            for mask in far + near:
                hand_on(crossing[0], mask).wait_recv()

            def pieces_at(row, col):
                window = (slice(None), slice(row, row + 8), slice(col, col + lanes))
                return [
                    passed[(mask,) + window]
                    if mask == 0
                    else arrived[(crossing[0], mask - 1) + window]
                    for mask in range(depth_count)
                ]

            def put(row, col, total):
                at = pl.ds(pl.multiple_of(there * cols + col, lanes), lanes)
                for c in range(4):
                    out_ref[c, row : row + 8, at] = total[c]

            merge(pieces_at, fronts(there), put)

    def each(first, last, body):
        def step(n, carry):
            body(n)
            return carry

        lax.fori_loop(first, last, step, 0)

    lag = min(LAG, units)
    for at, mask in enumerate(far + near):
        fetch(steps[0], mask).wait()
        if at == 0:
            fetch_rest()
        march(steps[0], mask, sent.at[steps[0], mask - 1])
        if at == 0:
            pl.semaphore_wait(barrier, depth_count - 1 + beside)
            if rounds:
                greet(pass_sem.at[0])
        send(steps[0], mask).start()
    each(1, HEAD, feed)
    widen(0, 1)
    cross()
    widen(1, 2)
    each(HEAD, lag, feed)
    widen(2, rounds)

    def advance(n, carry):
        blend(n - lag)

        @pl.when(n < units)
        def _():
            feed(n)

        return carry

    lax.fori_loop(lag, units + lag, advance, 0)
    here = pl.ds(pl.multiple_of(tile * cols, lanes), cols)
    out_ref[:, :, here] = merged[0, own_place]

    late = [mask for mask in range(tile_count - 1, 0, -1) if mask not in crossing]
    for mask in late:
        take_row(mask).wait_recv()
    for step in steps:
        for mask in range(1, depth_count):
            send(step, mask).wait_send()
    for step in crossing:
        for mask in range(depth_count):
            carry_over(step, mask).wait_send()
    for mask in late:
        send_row(mask // owners, mask % owners).wait_send()


def local(voxel_bins, colors, opacity, slab_order):
    depth_count = lax.axis_size("depth")
    tile_count = lax.axis_size("screen")
    samples, row_count, cols = voxel_bins.shape
    rows_each = row_count // (depth_count * tile_count)
    unit_rows = max(8, rows_each)
    owners = unit_rows // rows_each
    units = tile_count // owners
    rate = extinction / (samples * depth_count)
    sizes = (depth_count, tile_count, samples, unit_rows, units, owners, rows_each, cols, rate)
    others = depth_count - 1
    vmem = pl.BlockSpec(memory_space=pltpu.VMEM)
    return pl.pallas_call(
        functools.partial(kernel, sizes),
        out_shape=pltpu.VMEM((4, rows_each, cols * tile_count), jnp.float32),
        in_specs=[
            pl.BlockSpec(memory_space=pltpu.SMEM),
            pl.BlockSpec(memory_space=pl.ANY),
            vmem,
            vmem,
        ],
        out_specs=vmem,
        scratch_shapes=[
            pltpu.VMEM((units, depth_count, samples, unit_rows, cols), jnp.int32),
            pltpu.VMEM((units, others, 4, unit_rows, cols), jnp.float32),
            pltpu.VMEM((units, 4, unit_rows, cols), jnp.float32),
            pltpu.VMEM((units, others, 4, unit_rows, cols), jnp.float32),
            pltpu.VMEM((units, owners, 4, rows_each, cols), jnp.float32),
            pltpu.SemaphoreType.DMA((units, depth_count)),
            pltpu.SemaphoreType.DMA((units, others)),
            pltpu.SemaphoreType.DMA((units, others)),
            pltpu.SemaphoreType.DMA((tile_count,)),
            pltpu.SemaphoreType.DMA((tile_count,)),
            pltpu.SemaphoreType.REGULAR((tile_count,)),
            pltpu.VMEM((depth_count, 4, unit_rows, cols), jnp.float32),
            pltpu.SemaphoreType.DMA((depth_count,)),
            pltpu.SemaphoreType.DMA((depth_count,)),
        ],
        compiler_params=pltpu.CompilerParams(collective_id=0, has_side_effects=True),
    )(slab_order.T, voxel_bins, colors, opacity)


def solution(mesh):
    placed = (P("depth", None, "screen"), P(), P(), P())
    return jax.shard_map(
        local,
        mesh=mesh,
        in_specs=placed,
        out_specs=P(None, ("depth", "screen"), None),
        check_vma=False,
    )
```

```python
import functools

import jax
import jax.numpy as jnp
from jax import lax
from jax.experimental import pallas as pl
from jax.experimental.pallas import tpu as pltpu
from jax.sharding import PartitionSpec as P

extinction = 3.0
lanes = 128
HEAD, LAG = 2, 4
MESH = pl.DeviceIdType.MESH


def flip(index, mask, count):
    result = index
    bit = 1
    while bit < count:
        if isinstance(mask, int):
            if mask & bit:
                result = result + bit * (1 - 2 * lax.rem(lax.div(index, bit), 2))
        else:
            mine = lax.rem(lax.div(index, bit), 2)
            other = lax.rem(lax.div(mask, bit), 2)
            result = result + bit * other * (1 - 2 * mine)
        bit *= 2
    return result


def kernel(
    sizes,
    order_hbm,
    bins_hbm,
    colors_hbm,
    opacity_hbm,
    out_ref,
    order_ref,
    colors_ref,
    opacity_ref,
    table_sem,
    bins,
    sent,
    own,
    arrived,
    merged,
    bins_sem,
    send_sem,
    recv_sem,
    row_send_sem,
    row_recv_sem,
    pass_sem,
    passed,
    pass_send_sem,
    pass_recv_sem,
):
    depth_count, tile_count, samples, unit_rows, units, owners, rows_each, cols, rate = sizes
    depth = lax.axis_index("depth")
    tile = lax.axis_index("screen")
    own_unit = lax.div(tile, owners)
    own_place = lax.rem(tile, owners)
    steps = list(range(units - 1, -1, -1))
    crossing = [2] if owners == 1 and units > 3 else []
    peers = [depth_count - 1] + list(range(1, depth_count - 1)) + [0]

    barrier = pltpu.get_barrier_semaphore()
    near = [mask for mask in peers if mask and not mask & (mask - 1)]
    far = [mask for mask in peers if mask & (mask - 1)]
    below = tile >= 2
    above = tile + 2 < tile_count
    beside = 1 + below.astype(jnp.int32) + above.astype(jnp.int32)

    def greet(sem):
        def tell(there):
            pl.semaphore_signal(sem, inc=1, device_id=(depth, there), device_id_type=MESH)

        tell(flip(tile, 1, tile_count))

        @pl.when(below)
        def _():
            tell(tile - 2)

        @pl.when(above)
        def _():
            tell(tile + 2)

    rounds = tile_count // 2 - 1

    def widen(first, last):
        for n in range(first, min(last, rounds)):
            pl.semaphore_wait(pass_sem.at[n], beside)
            if n + 1 < rounds:
                greet(pass_sem.at[n + 1])

    for mask in far + near:
        peer = flip(depth, mask, depth_count)
        pl.semaphore_signal(barrier, inc=1, device_id=(peer, tile), device_id_type=MESH)
    greet(barrier)

    def fetch(step, mask):
        row = (flip(depth, mask, depth_count) * units + flip(own_unit, step, units)) * unit_rows
        row = pl.multiple_of(row, unit_rows)
        return pltpu.make_async_copy(
            bins_hbm.at[:, pl.ds(row, unit_rows), :],
            bins.at[step, mask],
            bins_sem.at[step, mask],
        )

    loads = [
        pltpu.make_async_copy(colors_hbm, colors_ref, table_sem.at[0]),
        pltpu.make_async_copy(opacity_hbm, opacity_ref, table_sem.at[1]),
        pltpu.make_async_copy(order_hbm, order_ref, table_sem.at[2]),
    ]
    for load in loads:
        load.start()
    for mask in far + near:
        fetch(steps[0], mask).start()

    def fetch_rest():
        for step in steps[1:2] + crossing + [k for k in steps[2:] if k not in crossing]:
            for mask in far + near:
                fetch(step, mask).start()
        for step in crossing + [k for k in steps if k not in crossing]:
            fetch(step, 0).start()

    for load in loads:
        load.wait()
    density = opacity_ref[...].astype(jnp.float32).reshape(1, -1)
    weight = 1.0 - jnp.exp(-rate * density)
    shades = weight * colors_ref[...].astype(jnp.float32)
    table = [shades[c : c + 1] for c in range(3)] + [weight]
    bin_count = weight.shape[1]
    parts = [
        [jnp.broadcast_to(row[:, at : at + lanes], (8, lanes)) for at in range(0, bin_count, lanes)]
        for row in table
    ]

    def march(step, mask, target):
        for row in range(0, unit_rows, 8):
            for col in range(0, cols, lanes):
                clear = None
                total = None
                for j in range(samples):
                    index = bins[step, mask, j, row : row + 8, col : col + lanes]
                    low = lax.rem(index, lanes) if lanes & (lanes - 1) else index & (lanes - 1)
                    values = []
                    for part in parts:
                        value = jnp.take_along_axis(part[0], low, axis=1, mode="promise_in_bounds")
                        for n in range(1, len(part)):
                            other = jnp.take_along_axis(
                                part[n], low, axis=1, mode="promise_in_bounds"
                            )
                            value = jnp.where(index >= n * lanes, other, value)
                        values.append(value)
                    if total is None:
                        total = values
                        clear = 1.0 - values[3]
                    else:
                        seen = clear * values[3]
                        total = [t + clear * v for t, v in zip(total[:3], values[:3])] + [
                            total[3] + seen
                        ]
                        clear = clear - seen
                for c in range(4):
                    target[c, row : row + 8, col : col + lanes] = total[c]

    def send(step, mask):
        return pltpu.make_async_remote_copy(
            src_ref=sent.at[step, mask - 1],
            dst_ref=arrived.at[step, mask - 1],
            send_sem=send_sem.at[step, mask - 1],
            recv_sem=recv_sem.at[step, mask - 1],
            device_id=(flip(depth, mask, depth_count), tile),
            device_id_type=MESH,
        )

    def send_row(step, low):
        mask = step * owners + low
        place = flip(own_place, low, owners)
        there = pl.ds(pl.multiple_of(tile * cols, lanes), cols)
        return pltpu.make_async_remote_copy(
            src_ref=merged.at[step, place],
            dst_ref=out_ref.at[:, :, there],
            send_sem=row_send_sem.at[mask],
            recv_sem=row_recv_sem.at[mask],
            device_id=(depth, flip(tile, mask, tile_count)),
            device_id_type=MESH,
        )

    def take_row(mask):
        here = pl.ds(pl.multiple_of(flip(tile, mask, tile_count) * cols, lanes), cols)
        return pltpu.make_async_remote_copy(
            src_ref=merged.at[0, 0],
            dst_ref=out_ref.at[:, :, here],
            send_sem=row_send_sem.at[mask],
            recv_sem=row_recv_sem.at[mask],
            device_id=(depth, flip(tile, mask, tile_count)),
            device_id_type=MESH,
        )

    def carry_over(step, mask):
        return pltpu.make_async_remote_copy(
            src_ref=sent.at[step, mask - 1] if mask else own.at[step],
            dst_ref=passed.at[mask],
            send_sem=pass_send_sem.at[mask],
            recv_sem=pass_recv_sem.at[mask],
            device_id=(depth, flip(tile, step, tile_count)),
            device_id_type=MESH,
        )

    def hand_on(step, mask):
        return pltpu.make_async_remote_copy(
            src_ref=passed.at[mask],
            dst_ref=arrived.at[step, mask - 1],
            send_sem=send_sem.at[step, mask - 1],
            recv_sem=recv_sem.at[step, mask - 1],
            device_id=(flip(depth, mask, depth_count), tile),
            device_id_type=MESH,
        )

    def cross():
        for step in crossing:
            for mask in far + near + [0]:
                fetch(step, mask).wait()
                march(step, mask, sent.at[step, mask - 1] if mask else own.at[step])
                carry_over(step, mask).start()

    def feed(n):
        step = units - 1 - n

        def plain():
            for mask in far + near:
                fetch(step, mask).wait()
                march(step, mask, sent.at[step, mask - 1])
                send(step, mask).start()

        if not crossing:
            plain()
            return
        pl.when(step != crossing[0])(plain)

        @pl.when(step == crossing[0])
        def _():
            for mask in far + near:
                carry_over(crossing[0], mask).wait_recv()
                hand_on(crossing[0], mask).start()

    def fronts(of_tile):
        place_of = [
            order_ref[flip(depth, mask, depth_count), of_tile] for mask in range(depth_count)
        ]
        return [
            [jnp.where(place_of[j] < place_of[i], 1.0, 0.0) for j in range(depth_count)]
            for i in range(depth_count)
        ]

    def merge(pieces_at, ahead, put):
        for row in range(0, unit_rows, 8):
            for col in range(0, cols, lanes):
                pieces = pieces_at(row, col)
                total = None
                for i in range(depth_count):
                    front = None
                    for j in range(depth_count):
                        if j != i:
                            clear = 1.0 - ahead[i][j] * pieces[j][3]
                            front = clear if front is None else front * clear
                    lit = [pieces[i][c] if front is None else pieces[i][c] * front for c in range(4)]
                    total = lit if total is None else [t + v for t, v in zip(total, lit)]
                put(row, col, total)

    ahead = fronts(tile)

    def blend(n):
        step = units - 1 - n

        def plain():
            fetch(step, 0).wait()
            march(step, 0, own.at[step])
            for mask in far + near:
                send(step, mask).wait_recv()

            def pieces_at(row, col):
                window = (slice(None), slice(row, row + 8), slice(col, col + lanes))
                return [
                    own[(step,) + window] if mask == 0 else arrived[(step, mask - 1) + window]
                    for mask in range(depth_count)
                ]

            def put(row, col, total):
                for c in range(4):
                    if owners == 1:
                        merged[step, 0, c, row : row + 8, col : col + lanes] = total[c]
                    else:
                        for place in range(owners):
                            merged[step, place, c, :, col : col + lanes] = total[c][
                                place * rows_each : (place + 1) * rows_each
                            ]

            merge(pieces_at, ahead, put)
            for low in range(owners - 1, 0, -1):
                send_row(step, low).start()

            @pl.when(step > 0)
            def _():
                send_row(step, 0).start()

        if not crossing:
            plain()
            return
        pl.when(step != crossing[0])(plain)

        @pl.when(step == crossing[0])
        def _():
            there = flip(tile, crossing[0], tile_count)
            carry_over(crossing[0], 0).wait_recv()
            for mask in far + near:
                hand_on(crossing[0], mask).wait_recv()

            def pieces_at(row, col):
                window = (slice(None), slice(row, row + 8), slice(col, col + lanes))
                return [
                    passed[(mask,) + window]
                    if mask == 0
                    else arrived[(crossing[0], mask - 1) + window]
                    for mask in range(depth_count)
                ]

            def put(row, col, total):
                at = pl.ds(pl.multiple_of(there * cols + col, lanes), lanes)
                for c in range(4):
                    out_ref[c, row : row + 8, at] = total[c]

            merge(pieces_at, fronts(there), put)

    def each(first, last, body):
        def step(n, carry):
            body(n)
            return carry

        lax.fori_loop(first, last, step, 0)

    lag = min(LAG, units)
    for at, mask in enumerate(far + near):
        fetch(steps[0], mask).wait()
        if at == 0:
            fetch_rest()
        march(steps[0], mask, sent.at[steps[0], mask - 1])
        if at == 0:
            pl.semaphore_wait(barrier, depth_count - 1 + beside)
            if rounds:
                greet(pass_sem.at[0])
        send(steps[0], mask).start()
    each(1, HEAD, feed)
    widen(0, 1)
    cross()
    widen(1, 2)
    each(HEAD, lag, feed)
    widen(2, rounds)

    def advance(n, carry):
        blend(n - lag)

        @pl.when(n < units)
        def _():
            feed(n)

        return carry

    lax.fori_loop(lag, units + lag, advance, 0)
    here = pl.ds(pl.multiple_of(tile * cols, lanes), cols)
    out_ref[:, :, here] = merged[0, own_place]

    late = [mask for mask in range(tile_count - 1, 0, -1) if mask not in crossing]
    for mask in late:
        take_row(mask).wait_recv()
    for step in steps:
        for mask in range(1, depth_count):
            send(step, mask).wait_send()
    for step in crossing:
        for mask in range(depth_count):
            carry_over(step, mask).wait_send()
    for mask in late:
        send_row(mask // owners, mask % owners).wait_send()


def local(voxel_bins, colors, opacity, slab_order):
    depth_count = lax.axis_size("depth")
    tile_count = lax.axis_size("screen")
    samples, row_count, cols = voxel_bins.shape
    rows_each = row_count // (depth_count * tile_count)
    unit_rows = max(8, rows_each)
    owners = unit_rows // rows_each
    units = tile_count // owners
    rate = extinction / (samples * depth_count)
    sizes = (depth_count, tile_count, samples, unit_rows, units, owners, rows_each, cols, rate)
    others = depth_count - 1
    return pl.pallas_call(
        functools.partial(kernel, sizes),
        out_shape=pltpu.VMEM((4, rows_each, cols * tile_count), jnp.float32),
        in_specs=[pl.BlockSpec(memory_space=pl.ANY)] * 4,
        out_specs=pl.BlockSpec(memory_space=pltpu.VMEM),
        scratch_shapes=[
            pltpu.SMEM(slab_order.shape[::-1], slab_order.dtype),
            pltpu.VMEM(colors.shape, colors.dtype),
            pltpu.VMEM(opacity.shape, opacity.dtype),
            pltpu.SemaphoreType.DMA((3,)),
            pltpu.VMEM((units, depth_count, samples, unit_rows, cols), jnp.int32),
            pltpu.VMEM((units, others, 4, unit_rows, cols), jnp.float32),
            pltpu.VMEM((units, 4, unit_rows, cols), jnp.float32),
            pltpu.VMEM((units, others, 4, unit_rows, cols), jnp.float32),
            pltpu.VMEM((units, owners, 4, rows_each, cols), jnp.float32),
            pltpu.SemaphoreType.DMA((units, depth_count)),
            pltpu.SemaphoreType.DMA((units, others)),
            pltpu.SemaphoreType.DMA((units, others)),
            pltpu.SemaphoreType.DMA((tile_count,)),
            pltpu.SemaphoreType.DMA((tile_count,)),
            pltpu.SemaphoreType.REGULAR((tile_count,)),
            pltpu.VMEM((depth_count, 4, unit_rows, cols), jnp.float32),
            pltpu.SemaphoreType.DMA((depth_count,)),
            pltpu.SemaphoreType.DMA((depth_count,)),
        ],
        compiler_params=pltpu.CompilerParams(collective_id=0, has_side_effects=True),
    )(slab_order.T, voxel_bins, colors, opacity)


def solution(mesh):
    placed = (P("depth", None, "screen"), P(), P(), P())
    return jax.shard_map(
        local,
        mesh=mesh,
        in_specs=placed,
        out_specs=P(None, ("depth", "screen"), None),
        check_vma=False,
    )
```

```python
import functools

import jax
import jax.numpy as jnp
from jax import lax
from jax.experimental import pallas as pl
from jax.experimental.pallas import tpu as pltpu
from jax.sharding import PartitionSpec as P

extinction = 3.0
lanes = 128
HEAD, LAG, PRE = 3, 4, (6, 3, 1)
MESH = pl.DeviceIdType.MESH


def flip(index, mask, count):
    result = index
    bit = 1
    while bit < count:
        if isinstance(mask, int):
            if mask & bit:
                result = result + bit * (1 - 2 * lax.rem(lax.div(index, bit), 2))
        else:
            mine = lax.rem(lax.div(index, bit), 2)
            other = lax.rem(lax.div(mask, bit), 2)
            result = result + bit * other * (1 - 2 * mine)
        bit *= 2
    return result


def kernel(
    sizes,
    order_hbm,
    bins_hbm,
    colors_hbm,
    opacity_hbm,
    out_ref,
    order_ref,
    colors_ref,
    opacity_ref,
    table_sem,
    bins,
    sent,
    own,
    arrived,
    merged,
    bins_sem,
    send_sem,
    recv_sem,
    row_send_sem,
    row_recv_sem,
    pass_sem,
    passed,
    pass_send_sem,
    pass_recv_sem,
):
    depth_count, tile_count, samples, unit_rows, units, owners, rows_each, cols, rate = sizes
    depth = lax.axis_index("depth")
    tile = lax.axis_index("screen")
    own_unit = lax.div(tile, owners)
    own_place = lax.rem(tile, owners)
    crossing = [2] if owners == 1 and units > 3 else []
    steps = [step for step in range(units - 1, -1, -1) if step not in crossing] + crossing

    def step_of(n):
        if not crossing:
            return units - 1 - n
        kept = jnp.where(n < units - 1 - crossing[0], units - 1 - n, units - 2 - n)
        return jnp.where(n == units - 1, crossing[0], kept)

    peers = [depth_count - 1] + list(range(1, depth_count - 1)) + [0]

    barrier = pltpu.get_barrier_semaphore()
    near = [mask for mask in peers if mask and not mask & (mask - 1)]
    far = [mask for mask in peers if mask & (mask - 1)]
    below = tile >= 2
    above = tile + 2 < tile_count
    beside = 1 + below.astype(jnp.int32) + above.astype(jnp.int32)

    def greet(sem):
        def tell(there):
            pl.semaphore_signal(sem, inc=1, device_id=(depth, there), device_id_type=MESH)

        tell(flip(tile, 1, tile_count))

        @pl.when(below)
        def _():
            tell(tile - 2)

        @pl.when(above)
        def _():
            tell(tile + 2)

    rounds = tile_count // 2 - 1

    def widen(first, last):
        for n in range(first, min(last, rounds)):
            pl.semaphore_wait(pass_sem.at[n], beside)
            if n + 1 < rounds:
                greet(pass_sem.at[n + 1])

    for mask in far + near:
        peer = flip(depth, mask, depth_count)
        pl.semaphore_signal(barrier, inc=1, device_id=(peer, tile), device_id_type=MESH)
    greet(barrier)

    def fetch(step, mask):
        row = (flip(depth, mask, depth_count) * units + flip(own_unit, step, units)) * unit_rows
        row = pl.multiple_of(row, unit_rows)
        return pltpu.make_async_copy(
            bins_hbm.at[:, pl.ds(row, unit_rows), :],
            bins.at[step, mask],
            bins_sem.at[step, mask],
        )

    loads = [
        pltpu.make_async_copy(colors_hbm, colors_ref, table_sem.at[0]),
        pltpu.make_async_copy(opacity_hbm, opacity_ref, table_sem.at[1]),
        pltpu.make_async_copy(order_hbm, order_ref, table_sem.at[2]),
    ]
    for load in loads:
        load.start()
    for mask in far + near:
        fetch(steps[0], mask).start()

    def fetch_rest():
        for step in steps[1:2] + crossing + [k for k in steps[2:] if k not in crossing]:
            for mask in far + near:
                fetch(step, mask).start()
        for step in crossing + [k for k in steps if k not in crossing]:
            fetch(step, 0).start()

    for load in loads:
        load.wait()
    density = opacity_ref[...].astype(jnp.float32).reshape(1, -1)
    weight = 1.0 - jnp.exp(-rate * density)
    shades = weight * colors_ref[...].astype(jnp.float32)
    table = [shades[c : c + 1] for c in range(3)] + [weight]
    bin_count = weight.shape[1]
    parts = [
        [jnp.broadcast_to(row[:, at : at + lanes], (8, lanes)) for at in range(0, bin_count, lanes)]
        for row in table
    ]

    def march(step, mask, target):
        for row in range(0, unit_rows, 8):
            for col in range(0, cols, lanes):
                clear = None
                total = None
                for j in range(samples):
                    index = bins[step, mask, j, row : row + 8, col : col + lanes]
                    low = lax.rem(index, lanes) if lanes & (lanes - 1) else index & (lanes - 1)
                    values = []
                    for part in parts:
                        value = jnp.take_along_axis(part[0], low, axis=1, mode="promise_in_bounds")
                        for n in range(1, len(part)):
                            other = jnp.take_along_axis(
                                part[n], low, axis=1, mode="promise_in_bounds"
                            )
                            value = jnp.where(index >= n * lanes, other, value)
                        values.append(value)
                    if total is None:
                        total = values
                        clear = 1.0 - values[3]
                    else:
                        seen = clear * values[3]
                        total = [t + clear * v for t, v in zip(total[:3], values[:3])] + [
                            total[3] + seen
                        ]
                        clear = clear - seen
                for c in range(4):
                    target[c, row : row + 8, col : col + lanes] = total[c]

    def send(step, mask):
        return pltpu.make_async_remote_copy(
            src_ref=sent.at[step, mask - 1],
            dst_ref=arrived.at[step, mask - 1],
            send_sem=send_sem.at[step, mask - 1],
            recv_sem=recv_sem.at[step, mask - 1],
            device_id=(flip(depth, mask, depth_count), tile),
            device_id_type=MESH,
        )

    def send_row(step, low):
        mask = step * owners + low
        place = flip(own_place, low, owners)
        there = pl.ds(pl.multiple_of(tile * cols, lanes), cols)
        return pltpu.make_async_remote_copy(
            src_ref=merged.at[step, place],
            dst_ref=out_ref.at[:, :, there],
            send_sem=row_send_sem.at[mask],
            recv_sem=row_recv_sem.at[mask],
            device_id=(depth, flip(tile, mask, tile_count)),
            device_id_type=MESH,
        )

    def take_row(mask):
        here = pl.ds(pl.multiple_of(flip(tile, mask, tile_count) * cols, lanes), cols)
        return pltpu.make_async_remote_copy(
            src_ref=merged.at[0, 0],
            dst_ref=out_ref.at[:, :, here],
            send_sem=row_send_sem.at[mask],
            recv_sem=row_recv_sem.at[mask],
            device_id=(depth, flip(tile, mask, tile_count)),
            device_id_type=MESH,
        )

    def carry_over(step, mask):
        return pltpu.make_async_remote_copy(
            src_ref=sent.at[step, mask - 1] if mask else own.at[step],
            dst_ref=passed.at[mask],
            send_sem=pass_send_sem.at[mask],
            recv_sem=pass_recv_sem.at[mask],
            device_id=(depth, flip(tile, step, tile_count)),
            device_id_type=MESH,
        )

    def hand_on(step, mask):
        return pltpu.make_async_remote_copy(
            src_ref=passed.at[mask],
            dst_ref=arrived.at[step, mask - 1],
            send_sem=send_sem.at[step, mask - 1],
            recv_sem=recv_sem.at[step, mask - 1],
            device_id=(flip(depth, mask, depth_count), tile),
            device_id_type=MESH,
        )

    def cross():
        for step in crossing:
            for mask in far + near + [0]:
                fetch(step, mask).wait()
                march(step, mask, sent.at[step, mask - 1] if mask else own.at[step])
                carry_over(step, mask).start()

    def feed(n):
        step = step_of(n)

        def plain():
            for mask in far + near:
                fetch(step, mask).wait()
                march(step, mask, sent.at[step, mask - 1])
                send(step, mask).start()

        if not crossing:
            plain()
            return
        pl.when(step != crossing[0])(plain)

        @pl.when(step == crossing[0])
        def _():
            for mask in far + near:
                carry_over(crossing[0], mask).wait_recv()
                hand_on(crossing[0], mask).start()

    def fronts(of_tile):
        place_of = [
            order_ref[flip(depth, mask, depth_count), of_tile] for mask in range(depth_count)
        ]
        return [
            [jnp.where(place_of[j] < place_of[i], 1.0, 0.0) for j in range(depth_count)]
            for i in range(depth_count)
        ]

    def merge(pieces_at, ahead, put):
        for row in range(0, unit_rows, 8):
            for col in range(0, cols, lanes):
                pieces = pieces_at(row, col)
                total = None
                for i in range(depth_count):
                    front = None
                    for j in range(depth_count):
                        if j != i:
                            clear = 1.0 - ahead[i][j] * pieces[j][3]
                            front = clear if front is None else front * clear
                    lit = [pieces[i][c] if front is None else pieces[i][c] * front for c in range(4)]
                    total = lit if total is None else [t + v for t, v in zip(total, lit)]
                put(row, col, total)

    ahead = fronts(tile)

    def blend(n):
        step = step_of(n)

        def plain():
            fetch(step, 0).wait()
            march(step, 0, own.at[step])
            for mask in far + near:
                send(step, mask).wait_recv()

            def pieces_at(row, col):
                window = (slice(None), slice(row, row + 8), slice(col, col + lanes))
                return [
                    own[(step,) + window] if mask == 0 else arrived[(step, mask - 1) + window]
                    for mask in range(depth_count)
                ]

            def put(row, col, total):
                for c in range(4):
                    if owners == 1:
                        merged[step, 0, c, row : row + 8, col : col + lanes] = total[c]
                    else:
                        for place in range(owners):
                            merged[step, place, c, :, col : col + lanes] = total[c][
                                place * rows_each : (place + 1) * rows_each
                            ]

            merge(pieces_at, ahead, put)
            for low in range(owners - 1, 0, -1):
                send_row(step, low).start()

            @pl.when(step > 0)
            def _():
                send_row(step, 0).start()

        if not crossing:
            plain()
            return
        pl.when(step != crossing[0])(plain)

        @pl.when(step == crossing[0])
        def _():
            there = flip(tile, crossing[0], tile_count)
            carry_over(crossing[0], 0).wait_recv()
            for mask in far + near:
                hand_on(crossing[0], mask).wait_recv()

            def pieces_at(row, col):
                window = (slice(None), slice(row, row + 8), slice(col, col + lanes))
                return [
                    passed[(mask,) + window]
                    if mask == 0
                    else arrived[(crossing[0], mask - 1) + window]
                    for mask in range(depth_count)
                ]

            def put(row, col, total):
                at = pl.ds(pl.multiple_of(there * cols + col, lanes), lanes)
                for c in range(4):
                    out_ref[c, row : row + 8, at] = total[c]

            merge(pieces_at, fronts(there), put)

    def each(first, last, body):
        def step(n, carry):
            body(n)
            return carry

        lax.fori_loop(first, last, step, 0)

    lag = min(LAG, units)
    ones = sum(lax.rem(lax.div(depth, bit), 2) for bit in near)
    ready = jnp.where(ones == 0, PRE[0], jnp.where(ones == len(near), PRE[2], PRE[1]))
    opening = [(step, mask) for step in steps[:2] for mask in far + near]
    for at, piece in enumerate(opening):
        fetch(*piece).wait()
        if at == 0:
            fetch_rest()
        march(*piece, sent.at[piece[0], piece[1] - 1])

        @pl.when(ready == at + 1)
        def _():
            pl.semaphore_wait(barrier, depth_count - 1 + beside)
            if rounds:
                greet(pass_sem.at[0])
            for earlier in opening[: at + 1]:
                send(*earlier).start()

        @pl.when(ready < at + 1)
        def _():
            send(*piece).start()

    each(2, HEAD, feed)
    widen(0, 1)
    cross()
    widen(1, 2)
    each(HEAD, lag, feed)
    widen(2, rounds)

    def advance(n, carry):
        blend(n - lag)

        @pl.when(n < units)
        def _():
            feed(n)

        return carry

    lax.fori_loop(lag, units + lag, advance, 0)
    here = pl.ds(pl.multiple_of(tile * cols, lanes), cols)
    out_ref[:, :, here] = merged[0, own_place]

    late = [mask for mask in range(tile_count - 1, 0, -1) if mask not in crossing]
    for mask in late:
        take_row(mask).wait_recv()
    for step in steps:
        for mask in range(1, depth_count):
            send(step, mask).wait_send()
    for step in crossing:
        for mask in range(depth_count):
            carry_over(step, mask).wait_send()
    for mask in late:
        send_row(mask // owners, mask % owners).wait_send()


def local(voxel_bins, colors, opacity, slab_order):
    depth_count = lax.axis_size("depth")
    tile_count = lax.axis_size("screen")
    samples, row_count, cols = voxel_bins.shape
    rows_each = row_count // (depth_count * tile_count)
    unit_rows = max(8, rows_each)
    owners = unit_rows // rows_each
    units = tile_count // owners
    rate = extinction / (samples * depth_count)
    sizes = (depth_count, tile_count, samples, unit_rows, units, owners, rows_each, cols, rate)
    others = depth_count - 1
    return pl.pallas_call(
        functools.partial(kernel, sizes),
        out_shape=pltpu.VMEM((4, rows_each, cols * tile_count), jnp.float32),
        in_specs=[pl.BlockSpec(memory_space=pl.ANY)] * 4,
        out_specs=pl.BlockSpec(memory_space=pltpu.VMEM),
        scratch_shapes=[
            pltpu.SMEM(slab_order.shape[::-1], slab_order.dtype),
            pltpu.VMEM(colors.shape, colors.dtype),
            pltpu.VMEM(opacity.shape, opacity.dtype),
            pltpu.SemaphoreType.DMA((3,)),
            pltpu.VMEM((units, depth_count, samples, unit_rows, cols), jnp.int32),
            pltpu.VMEM((units, others, 4, unit_rows, cols), jnp.float32),
            pltpu.VMEM((units, 4, unit_rows, cols), jnp.float32),
            pltpu.VMEM((units, others, 4, unit_rows, cols), jnp.float32),
            pltpu.VMEM((units, owners, 4, rows_each, cols), jnp.float32),
            pltpu.SemaphoreType.DMA((units, depth_count)),
            pltpu.SemaphoreType.DMA((units, others)),
            pltpu.SemaphoreType.DMA((units, others)),
            pltpu.SemaphoreType.DMA((tile_count,)),
            pltpu.SemaphoreType.DMA((tile_count,)),
            pltpu.SemaphoreType.REGULAR((tile_count,)),
            pltpu.VMEM((depth_count, 4, unit_rows, cols), jnp.float32),
            pltpu.SemaphoreType.DMA((depth_count,)),
            pltpu.SemaphoreType.DMA((depth_count,)),
        ],
        compiler_params=pltpu.CompilerParams(collective_id=0, has_side_effects=True),
    )(slab_order.T, voxel_bins, colors, opacity)


def solution(mesh):
    placed = (P("depth", None, "screen"), P(), P(), P())
    return jax.shard_map(
        local,
        mesh=mesh,
        in_specs=placed,
        out_specs=P(None, ("depth", "screen"), None),
        check_vma=False,
    )
```

```python
import functools

import jax
import jax.numpy as jnp
from jax import lax
from jax.experimental import pallas as pl
from jax.experimental.pallas import tpu as pltpu
from jax.sharding import PartitionSpec as P

extinction = 3.0
lanes = 128
HEAD, LAG, PRE = 3, 4, (6, 3, 1)
MESH = pl.DeviceIdType.MESH


def flip(index, mask, count):
    result = index
    bit = 1
    while bit < count:
        if isinstance(mask, int):
            if mask & bit:
                result = result + bit * (1 - 2 * lax.rem(lax.div(index, bit), 2))
        else:
            mine = lax.rem(lax.div(index, bit), 2)
            other = lax.rem(lax.div(mask, bit), 2)
            result = result + bit * other * (1 - 2 * mine)
        bit *= 2
    return result


def kernel(
    sizes,
    order_hbm,
    bins_hbm,
    colors_hbm,
    opacity_hbm,
    out_ref,
    order_ref,
    colors_ref,
    opacity_ref,
    table_sem,
    bins,
    sent,
    own,
    arrived,
    merged,
    bins_sem,
    send_sem,
    recv_sem,
    row_send_sem,
    row_recv_sem,
    pass_sem,
    passed,
    pass_send_sem,
    pass_recv_sem,
):
    depth_count, tile_count, samples, unit_rows, units, owners, rows_each, cols, rate = sizes
    depth = lax.axis_index("depth")
    tile = lax.axis_index("screen")
    own_unit = lax.div(tile, owners)
    own_place = lax.rem(tile, owners)
    crossing = [2] if owners == 1 and units > 3 else []
    steps = [step for step in range(units - 1, -1, -1) if step not in crossing] + crossing

    def step_of(n):
        if not crossing:
            return units - 1 - n
        kept = jnp.where(n < units - 1 - crossing[0], units - 1 - n, units - 2 - n)
        return jnp.where(n == units - 1, crossing[0], kept)

    peers = [depth_count - 1] + list(range(1, depth_count - 1)) + [0]

    barrier = pltpu.get_barrier_semaphore()
    near = [mask for mask in peers if mask and not mask & (mask - 1)]
    far = [mask for mask in peers if mask & (mask - 1)]
    below = tile >= 2
    above = tile + 2 < tile_count
    beside = 1 + below.astype(jnp.int32) + above.astype(jnp.int32)

    def greet(sem):
        def tell(there):
            pl.semaphore_signal(sem, inc=1, device_id=(depth, there), device_id_type=MESH)

        tell(flip(tile, 1, tile_count))

        @pl.when(below)
        def _():
            tell(tile - 2)

        @pl.when(above)
        def _():
            tell(tile + 2)

    rounds = tile_count // 2 - 1

    def widen(first, last):
        for n in range(first, min(last, rounds)):
            pl.semaphore_wait(pass_sem.at[n], beside)
            if n + 1 < rounds:
                greet(pass_sem.at[n + 1])

    for mask in far + near:
        peer = flip(depth, mask, depth_count)
        pl.semaphore_signal(barrier, inc=1, device_id=(peer, tile), device_id_type=MESH)
    greet(barrier)

    def fetch(step, mask):
        row = (flip(depth, mask, depth_count) * units + flip(own_unit, step, units)) * unit_rows
        row = pl.multiple_of(row, unit_rows)
        return pltpu.make_async_copy(
            bins_hbm.at[:, pl.ds(row, unit_rows), :],
            bins.at[step, mask],
            bins_sem.at[step, mask],
        )

    loads = [
        pltpu.make_async_copy(colors_hbm, colors_ref, table_sem.at[0]),
        pltpu.make_async_copy(opacity_hbm, opacity_ref, table_sem.at[1]),
        pltpu.make_async_copy(order_hbm, order_ref, table_sem.at[2]),
    ]
    for load in loads:
        load.start()
    for mask in far + near:
        fetch(steps[0], mask).start()

    def fetch_rest():
        for step in steps[1:2] + crossing + [k for k in steps[2:] if k not in crossing]:
            for mask in far + near:
                fetch(step, mask).start()
        for step in crossing + [k for k in steps if k not in crossing]:
            fetch(step, 0).start()

    for load in loads:
        load.wait()
    density = opacity_ref[...].astype(jnp.float32).reshape(1, -1)
    weight = 1.0 - jnp.exp(-rate * density)
    shades = weight * colors_ref[...].astype(jnp.float32)
    table = [shades[c : c + 1] for c in range(3)] + [weight]
    bin_count = weight.shape[1]
    parts = [
        [jnp.broadcast_to(row[:, at : at + lanes], (8, lanes)) for at in range(0, bin_count, lanes)]
        for row in table
    ]

    def march(step, mask, target):
        for row in range(0, unit_rows, 8):
            for col in range(0, cols, lanes):
                clear = None
                total = None
                for j in range(samples):
                    index = bins[step, mask, j, row : row + 8, col : col + lanes]
                    low = lax.rem(index, lanes) if lanes & (lanes - 1) else index & (lanes - 1)
                    values = []
                    for part in parts:
                        value = jnp.take_along_axis(part[0], low, axis=1, mode="promise_in_bounds")
                        for n in range(1, len(part)):
                            other = jnp.take_along_axis(
                                part[n], low, axis=1, mode="promise_in_bounds"
                            )
                            value = jnp.where(index >= n * lanes, other, value)
                        values.append(value)
                    if total is None:
                        total = values
                        clear = 1.0 - values[3]
                    else:
                        seen = clear * values[3]
                        total = [t + clear * v for t, v in zip(total[:3], values[:3])] + [
                            total[3] + seen
                        ]
                        clear = clear - seen
                for c in range(4):
                    target[c, row : row + 8, col : col + lanes] = total[c]

    def send(step, mask):
        return pltpu.make_async_remote_copy(
            src_ref=sent.at[step, mask - 1],
            dst_ref=arrived.at[step, mask - 1],
            send_sem=send_sem.at[step, mask - 1],
            recv_sem=recv_sem.at[step, mask - 1],
            device_id=(flip(depth, mask, depth_count), tile),
            device_id_type=MESH,
        )

    def send_row(step, low):
        mask = step * owners + low
        place = flip(own_place, low, owners)
        there = pl.ds(pl.multiple_of(tile * cols, lanes), cols)
        return pltpu.make_async_remote_copy(
            src_ref=merged.at[step, place],
            dst_ref=out_ref.at[:, :, there],
            send_sem=row_send_sem.at[mask],
            recv_sem=row_recv_sem.at[mask],
            device_id=(depth, flip(tile, mask, tile_count)),
            device_id_type=MESH,
        )

    def take_row(mask):
        here = pl.ds(pl.multiple_of(flip(tile, mask, tile_count) * cols, lanes), cols)
        return pltpu.make_async_remote_copy(
            src_ref=merged.at[0, 0],
            dst_ref=out_ref.at[:, :, here],
            send_sem=row_send_sem.at[mask],
            recv_sem=row_recv_sem.at[mask],
            device_id=(depth, flip(tile, mask, tile_count)),
            device_id_type=MESH,
        )

    def carry_over(step, mask):
        return pltpu.make_async_remote_copy(
            src_ref=sent.at[step, mask - 1] if mask else own.at[step],
            dst_ref=passed.at[mask],
            send_sem=pass_send_sem.at[mask],
            recv_sem=pass_recv_sem.at[mask],
            device_id=(depth, flip(tile, step, tile_count)),
            device_id_type=MESH,
        )

    def hand_on(step, mask):
        return pltpu.make_async_remote_copy(
            src_ref=passed.at[mask],
            dst_ref=arrived.at[step, mask - 1],
            send_sem=send_sem.at[step, mask - 1],
            recv_sem=recv_sem.at[step, mask - 1],
            device_id=(flip(depth, mask, depth_count), tile),
            device_id_type=MESH,
        )

    def cross():
        for step in crossing:
            for mask in far + near + [0]:
                fetch(step, mask).wait()
            for mask in far + near + [0]:
                march(step, mask, sent.at[step, mask - 1] if mask else own.at[step])
                carry_over(step, mask).start()

    def give(n, masks):
        step = step_of(n)

        def plain():
            for mask in masks:
                fetch(step, mask).wait()
                march(step, mask, sent.at[step, mask - 1])
                send(step, mask).start()

        if not crossing:
            plain()
            return
        pl.when(step != crossing[0])(plain)

        @pl.when(step == crossing[0])
        def _():
            for mask in masks:
                carry_over(crossing[0], mask).wait_recv()
                hand_on(crossing[0], mask).start()

    def feed(n):
        give(n, far + near)

    def feed_ahead(n):
        @pl.when(n + 1 < units)
        def _():
            give(n + 1, far)

        give(n, near)

    def fronts(of_tile):
        place_of = [
            order_ref[flip(depth, mask, depth_count), of_tile] for mask in range(depth_count)
        ]
        return [
            [jnp.where(place_of[j] < place_of[i], 1.0, 0.0) for j in range(depth_count)]
            for i in range(depth_count)
        ]

    def merge(pieces_at, ahead, put):
        for row in range(0, unit_rows, 8):
            for col in range(0, cols, lanes):
                pieces = pieces_at(row, col)
                total = None
                for i in range(depth_count):
                    front = None
                    for j in range(depth_count):
                        if j != i:
                            clear = 1.0 - ahead[i][j] * pieces[j][3]
                            front = clear if front is None else front * clear
                    lit = [pieces[i][c] if front is None else pieces[i][c] * front for c in range(4)]
                    total = lit if total is None else [t + v for t, v in zip(total, lit)]
                put(row, col, total)

    ahead = fronts(tile)

    def blend(n):
        step = step_of(n)

        def plain():
            fetch(step, 0).wait()
            march(step, 0, own.at[step])
            for mask in far + near:
                send(step, mask).wait_recv()

            def pieces_at(row, col):
                window = (slice(None), slice(row, row + 8), slice(col, col + lanes))
                return [
                    own[(step,) + window] if mask == 0 else arrived[(step, mask - 1) + window]
                    for mask in range(depth_count)
                ]

            def put(row, col, total):
                for c in range(4):
                    if owners == 1:
                        merged[step, 0, c, row : row + 8, col : col + lanes] = total[c]
                    else:
                        for place in range(owners):
                            merged[step, place, c, :, col : col + lanes] = total[c][
                                place * rows_each : (place + 1) * rows_each
                            ]

            merge(pieces_at, ahead, put)
            for low in range(owners - 1, 0, -1):
                send_row(step, low).start()

            @pl.when(step > 0)
            def _():
                send_row(step, 0).start()

        if not crossing:
            plain()
            return
        pl.when(step != crossing[0])(plain)

        @pl.when(step == crossing[0])
        def _():
            there = flip(tile, crossing[0], tile_count)
            carry_over(crossing[0], 0).wait_recv()
            for mask in far + near:
                hand_on(crossing[0], mask).wait_recv()

            def pieces_at(row, col):
                window = (slice(None), slice(row, row + 8), slice(col, col + lanes))
                return [
                    passed[(mask,) + window]
                    if mask == 0
                    else arrived[(crossing[0], mask - 1) + window]
                    for mask in range(depth_count)
                ]

            def put(row, col, total):
                at = pl.ds(pl.multiple_of(there * cols + col, lanes), lanes)
                for c in range(4):
                    out_ref[c, row : row + 8, at] = total[c]

            merge(pieces_at, fronts(there), put)

    def each(first, last, body):
        def step(n, carry):
            body(n)
            return carry

        lax.fori_loop(first, last, step, 0)

    lag = min(LAG, units)
    ones = sum(lax.rem(lax.div(depth, bit), 2) for bit in near)
    ready = jnp.where(ones == 0, PRE[0], jnp.where(ones == len(near), PRE[2], PRE[1]))
    opening = [(step, mask) for step in steps[:2] for mask in far + near]
    for at, piece in enumerate(opening):
        fetch(*piece).wait()
        if at == 0:
            fetch_rest()
        march(*piece, sent.at[piece[0], piece[1] - 1])

        @pl.when(ready == at + 1)
        def _():
            pl.semaphore_wait(barrier, depth_count - 1 + beside)
            if rounds:
                greet(pass_sem.at[0])
            for earlier in opening[: at + 1]:
                send(*earlier).start()

        @pl.when(ready < at + 1)
        def _():
            send(*piece).start()

    each(2, HEAD, feed)
    widen(0, 1)
    cross()
    widen(1, 2)
    each(HEAD, lag, feed)
    give(min(lag, units - 1), far) if lag < units else None
    widen(2, rounds)

    def advance(n, carry):
        blend(n - lag)

        @pl.when(n < units)
        def _():
            feed_ahead(n)

        return carry

    lax.fori_loop(lag, units + lag, advance, 0)
    here = pl.ds(pl.multiple_of(tile * cols, lanes), cols)
    out_ref[:, :, here] = merged[0, own_place]

    late = [mask for mask in range(tile_count - 1, 0, -1) if mask not in crossing]
    for mask in late:
        take_row(mask).wait_recv()
    for step in steps:
        for mask in range(1, depth_count):
            send(step, mask).wait_send()
    for step in crossing:
        for mask in range(depth_count):
            carry_over(step, mask).wait_send()
    for mask in late:
        send_row(mask // owners, mask % owners).wait_send()


def local(voxel_bins, colors, opacity, slab_order):
    depth_count = lax.axis_size("depth")
    tile_count = lax.axis_size("screen")
    samples, row_count, cols = voxel_bins.shape
    rows_each = row_count // (depth_count * tile_count)
    unit_rows = max(8, rows_each)
    owners = unit_rows // rows_each
    units = tile_count // owners
    rate = extinction / (samples * depth_count)
    sizes = (depth_count, tile_count, samples, unit_rows, units, owners, rows_each, cols, rate)
    others = depth_count - 1
    return pl.pallas_call(
        functools.partial(kernel, sizes),
        out_shape=pltpu.VMEM((4, rows_each, cols * tile_count), jnp.float32),
        in_specs=[pl.BlockSpec(memory_space=pl.ANY)] * 4,
        out_specs=pl.BlockSpec(memory_space=pltpu.VMEM),
        scratch_shapes=[
            pltpu.SMEM(slab_order.shape[::-1], slab_order.dtype),
            pltpu.VMEM(colors.shape, colors.dtype),
            pltpu.VMEM(opacity.shape, opacity.dtype),
            pltpu.SemaphoreType.DMA((3,)),
            pltpu.VMEM((units, depth_count, samples, unit_rows, cols), jnp.int32),
            pltpu.VMEM((units, others, 4, unit_rows, cols), jnp.float32),
            pltpu.VMEM((units, 4, unit_rows, cols), jnp.float32),
            pltpu.VMEM((units, others, 4, unit_rows, cols), jnp.float32),
            pltpu.VMEM((units, owners, 4, rows_each, cols), jnp.float32),
            pltpu.SemaphoreType.DMA((units, depth_count)),
            pltpu.SemaphoreType.DMA((units, others)),
            pltpu.SemaphoreType.DMA((units, others)),
            pltpu.SemaphoreType.DMA((tile_count,)),
            pltpu.SemaphoreType.DMA((tile_count,)),
            pltpu.SemaphoreType.REGULAR((tile_count,)),
            pltpu.VMEM((depth_count, 4, unit_rows, cols), jnp.float32),
            pltpu.SemaphoreType.DMA((depth_count,)),
            pltpu.SemaphoreType.DMA((depth_count,)),
        ],
        compiler_params=pltpu.CompilerParams(collective_id=0, has_side_effects=True),
    )(slab_order.T, voxel_bins, colors, opacity)


def solution(mesh):
    placed = (P("depth", None, "screen"), P(), P(), P())
    return jax.shard_map(
        local,
        mesh=mesh,
        in_specs=placed,
        out_specs=P(None, ("depth", "screen"), None),
        check_vma=False,
    )
```

```python
import functools

import jax
import jax.numpy as jnp
from jax import lax
from jax.experimental import pallas as pl
from jax.experimental.pallas import tpu as pltpu
from jax.sharding import PartitionSpec as P

extinction = 3.0
lanes = 128
HEAD, LAG, PRE = 3, 4, (6, 3, 1)
MESH = pl.DeviceIdType.MESH


def flip(index, mask, count):
    result = index
    bit = 1
    while bit < count:
        if isinstance(mask, int):
            if mask & bit:
                result = result + bit * (1 - 2 * lax.rem(lax.div(index, bit), 2))
        else:
            mine = lax.rem(lax.div(index, bit), 2)
            other = lax.rem(lax.div(mask, bit), 2)
            result = result + bit * other * (1 - 2 * mine)
        bit *= 2
    return result


def kernel(
    sizes,
    order_hbm,
    bins_hbm,
    colors_hbm,
    opacity_hbm,
    out_ref,
    order_ref,
    colors_ref,
    opacity_ref,
    table_sem,
    bins,
    sent,
    own,
    arrived,
    merged,
    bins_sem,
    send_sem,
    recv_sem,
    row_send_sem,
    row_recv_sem,
    pass_sem,
    passed,
    pass_send_sem,
    pass_recv_sem,
):
    depth_count, tile_count, samples, unit_rows, units, owners, rows_each, cols, rate = sizes
    depth = lax.axis_index("depth")
    tile = lax.axis_index("screen")
    own_unit = lax.div(tile, owners)
    own_place = lax.rem(tile, owners)
    crossing = [2] if owners == 1 and units > 3 else []
    steps = [step for step in range(units - 1, -1, -1) if step not in crossing] + crossing

    def step_of(n):
        if not crossing:
            return units - 1 - n
        kept = jnp.where(n < units - 1 - crossing[0], units - 1 - n, units - 2 - n)
        return jnp.where(n == units - 1, crossing[0], kept)

    peers = [depth_count - 1] + list(range(1, depth_count - 1)) + [0]

    barrier = pltpu.get_barrier_semaphore()
    near = [mask for mask in peers if mask and not mask & (mask - 1)]
    far = [mask for mask in peers if mask & (mask - 1)]
    below = tile >= 2
    above = tile + 2 < tile_count
    beside = 1 + below.astype(jnp.int32) + above.astype(jnp.int32)

    def greet(sem):
        def tell(there):
            pl.semaphore_signal(sem, inc=1, device_id=(depth, there), device_id_type=MESH)

        tell(flip(tile, 1, tile_count))

        @pl.when(below)
        def _():
            tell(tile - 2)

        @pl.when(above)
        def _():
            tell(tile + 2)

    rounds = tile_count // 2 - 1

    def widen(first, last):
        for n in range(first, min(last, rounds)):
            pl.semaphore_wait(pass_sem.at[n], beside)
            if n + 1 < rounds:
                greet(pass_sem.at[n + 1])

    for mask in far + near:
        peer = flip(depth, mask, depth_count)
        pl.semaphore_signal(barrier, inc=1, device_id=(peer, tile), device_id_type=MESH)
    greet(barrier)

    def fetch(step, mask):
        row = (flip(depth, mask, depth_count) * units + flip(own_unit, step, units)) * unit_rows
        row = pl.multiple_of(row, unit_rows)
        return pltpu.make_async_copy(
            bins_hbm.at[:, pl.ds(row, unit_rows), :],
            bins.at[step, mask],
            bins_sem.at[step, mask],
        )

    loads = [
        pltpu.make_async_copy(colors_hbm, colors_ref, table_sem.at[0]),
        pltpu.make_async_copy(opacity_hbm, opacity_ref, table_sem.at[1]),
        pltpu.make_async_copy(order_hbm, order_ref, table_sem.at[2]),
    ]
    for load in loads:
        load.start()
    for mask in far + near:
        fetch(steps[0], mask).start()

    def fetch_rest():
        for step in steps[1:2] + crossing + [k for k in steps[2:] if k not in crossing]:
            for mask in far + near:
                fetch(step, mask).start()
        for step in crossing + [k for k in steps if k not in crossing]:
            fetch(step, 0).start()

    for load in loads:
        load.wait()
    density = opacity_ref[...].astype(jnp.float32).reshape(1, -1)
    weight = 1.0 - jnp.exp(-rate * density)
    shades = weight * colors_ref[...].astype(jnp.float32)
    table = [shades[c : c + 1] for c in range(3)] + [weight]
    bin_count = weight.shape[1]
    parts = [
        [jnp.broadcast_to(row[:, at : at + lanes], (8, lanes)) for at in range(0, bin_count, lanes)]
        for row in table
    ]

    def march(step, mask, target):
        for row in range(0, unit_rows, 8):
            for col in range(0, cols, lanes):
                clear = None
                total = None
                for j in range(samples):
                    index = bins[step, mask, j, row : row + 8, col : col + lanes]
                    low = lax.rem(index, lanes) if lanes & (lanes - 1) else index & (lanes - 1)
                    values = []
                    for part in parts:
                        value = jnp.take_along_axis(part[0], low, axis=1, mode="promise_in_bounds")
                        for n in range(1, len(part)):
                            other = jnp.take_along_axis(
                                part[n], low, axis=1, mode="promise_in_bounds"
                            )
                            value = jnp.where(index >= n * lanes, other, value)
                        values.append(value)
                    if total is None:
                        total = values
                        clear = 1.0 - values[3]
                    else:
                        seen = clear * values[3]
                        total = [t + clear * v for t, v in zip(total[:3], values[:3])] + [
                            total[3] + seen
                        ]
                        clear = clear - seen
                for c in range(4):
                    target[c, row : row + 8, col : col + lanes] = total[c]

    def send(step, mask):
        return pltpu.make_async_remote_copy(
            src_ref=sent.at[step, mask - 1],
            dst_ref=arrived.at[step, mask - 1],
            send_sem=send_sem.at[step, mask - 1],
            recv_sem=recv_sem.at[step, mask - 1],
            device_id=(flip(depth, mask, depth_count), tile),
            device_id_type=MESH,
        )

    def send_row(step, low):
        mask = step * owners + low
        place = flip(own_place, low, owners)
        there = pl.ds(pl.multiple_of(tile * cols, lanes), cols)
        return pltpu.make_async_remote_copy(
            src_ref=merged.at[step, place],
            dst_ref=out_ref.at[:, :, there],
            send_sem=row_send_sem.at[mask],
            recv_sem=row_recv_sem.at[mask],
            device_id=(depth, flip(tile, mask, tile_count)),
            device_id_type=MESH,
        )

    def take_row(mask):
        here = pl.ds(pl.multiple_of(flip(tile, mask, tile_count) * cols, lanes), cols)
        return pltpu.make_async_remote_copy(
            src_ref=merged.at[0, 0],
            dst_ref=out_ref.at[:, :, here],
            send_sem=row_send_sem.at[mask],
            recv_sem=row_recv_sem.at[mask],
            device_id=(depth, flip(tile, mask, tile_count)),
            device_id_type=MESH,
        )

    def carry_over(step, mask):
        return pltpu.make_async_remote_copy(
            src_ref=sent.at[step, mask - 1] if mask else own.at[step],
            dst_ref=passed.at[mask],
            send_sem=pass_send_sem.at[mask],
            recv_sem=pass_recv_sem.at[mask],
            device_id=(depth, flip(tile, step, tile_count)),
            device_id_type=MESH,
        )

    def hand_on(step, mask):
        return pltpu.make_async_remote_copy(
            src_ref=passed.at[mask],
            dst_ref=arrived.at[step, mask - 1],
            send_sem=send_sem.at[step, mask - 1],
            recv_sem=recv_sem.at[step, mask - 1],
            device_id=(flip(depth, mask, depth_count), tile),
            device_id_type=MESH,
        )

    def cross():
        for step in crossing:
            for mask in far + near + [0]:
                fetch(step, mask).wait()
            for mask in far + near + [0]:
                march(step, mask, sent.at[step, mask - 1] if mask else own.at[step])
                carry_over(step, mask).start()

    def give(n, masks):
        step = step_of(n)

        def plain():
            for mask in masks:
                fetch(step, mask).wait()
                march(step, mask, sent.at[step, mask - 1])
                send(step, mask).start()

        if not crossing:
            plain()
            return
        pl.when(step != crossing[0])(plain)

        @pl.when(step == crossing[0])
        def _():
            for mask in masks:
                carry_over(crossing[0], mask).wait_recv()
                hand_on(crossing[0], mask).start()

    def feed(n):
        give(n, far + near)

    def feed_ahead(n):
        @pl.when(n + 1 < units)
        def _():
            give(n + 1, far)

        give(n, near)

    def fronts(of_tile):
        place_of = [
            order_ref[flip(depth, mask, depth_count), of_tile] for mask in range(depth_count)
        ]
        return [
            [jnp.where(place_of[j] < place_of[i], 1.0, 0.0) for j in range(depth_count)]
            for i in range(depth_count)
        ]

    def merge(pieces_at, ahead, put):
        for row in range(0, unit_rows, 8):
            for col in range(0, cols, lanes):
                pieces = pieces_at(row, col)
                total = None
                for i in range(depth_count):
                    front = None
                    for j in range(depth_count):
                        if j != i:
                            clear = 1.0 - ahead[i][j] * pieces[j][3]
                            front = clear if front is None else front * clear
                    lit = [pieces[i][c] if front is None else pieces[i][c] * front for c in range(4)]
                    total = lit if total is None else [t + v for t, v in zip(total, lit)]
                put(row, col, total)

    ahead = fronts(tile)

    late = [mask for mask in range(tile_count - 1, 0, -1) if mask not in crossing]

    def settle():
        here = pl.ds(pl.multiple_of(tile * cols, lanes), cols)
        out_ref[:, :, here] = merged[0, own_place]
        for step in steps:
            for mask in range(1, depth_count):
                if step not in crossing:
                    send(step, mask).wait_send()
        for step in crossing:
            for mask in range(depth_count):
                carry_over(step, mask).wait_send()
        for mask in late:
            send_row(mask // owners, mask % owners).wait_send()

    def blend(n):
        step = step_of(n)

        def plain():
            fetch(step, 0).wait()
            march(step, 0, own.at[step])
            for mask in far + near:
                send(step, mask).wait_recv()

            def pieces_at(row, col):
                window = (slice(None), slice(row, row + 8), slice(col, col + lanes))
                return [
                    own[(step,) + window] if mask == 0 else arrived[(step, mask - 1) + window]
                    for mask in range(depth_count)
                ]

            def put(row, col, total):
                for c in range(4):
                    if owners == 1:
                        merged[step, 0, c, row : row + 8, col : col + lanes] = total[c]
                    else:
                        for place in range(owners):
                            merged[step, place, c, :, col : col + lanes] = total[c][
                                place * rows_each : (place + 1) * rows_each
                            ]

            merge(pieces_at, ahead, put)
            for low in range(owners - 1, 0, -1):
                send_row(step, low).start()

            @pl.when(step > 0)
            def _():
                send_row(step, 0).start()

        if not crossing:
            plain()
            return
        pl.when(step != crossing[0])(plain)

        @pl.when(step == crossing[0])
        def _():
            there = flip(tile, crossing[0], tile_count)
            settle()
            carry_over(crossing[0], 0).wait_recv()
            for mask in far + near:
                hand_on(crossing[0], mask).wait_recv()

            def pieces_at(row, col):
                window = (slice(None), slice(row, row + 8), slice(col, col + lanes))
                return [
                    passed[(mask,) + window]
                    if mask == 0
                    else arrived[(crossing[0], mask - 1) + window]
                    for mask in range(depth_count)
                ]

            def put(row, col, total):
                at = pl.ds(pl.multiple_of(there * cols + col, lanes), lanes)
                for c in range(4):
                    out_ref[c, row : row + 8, at] = total[c]

            merge(pieces_at, fronts(there), put)

    def each(first, last, body):
        def step(n, carry):
            body(n)
            return carry

        lax.fori_loop(first, last, step, 0)

    lag = min(LAG, units)
    ones = sum(lax.rem(lax.div(depth, bit), 2) for bit in near)
    ready = jnp.where(ones == 0, PRE[0], jnp.where(ones == len(near), PRE[2], PRE[1]))
    opening = [(step, mask) for step in steps[:2] for mask in far + near]
    for at, piece in enumerate(opening):
        fetch(*piece).wait()
        if at == 0:
            fetch_rest()
        march(*piece, sent.at[piece[0], piece[1] - 1])

        @pl.when(ready == at + 1)
        def _():
            pl.semaphore_wait(barrier, depth_count - 1 + beside)
            if rounds:
                greet(pass_sem.at[0])
            for earlier in opening[: at + 1]:
                send(*earlier).start()

        @pl.when(ready < at + 1)
        def _():
            send(*piece).start()

    each(2, HEAD, feed)
    widen(0, 1)
    cross()
    widen(1, 2)
    each(HEAD, lag, feed)
    give(min(lag, units - 1), far) if lag < units else None
    widen(2, rounds)

    def advance(n, carry):
        blend(n - lag)

        @pl.when(n < units)
        def _():
            feed_ahead(n)

        return carry

    lax.fori_loop(lag, units + lag, advance, 0)
    if not crossing:
        settle()
    for mask in late:
        take_row(mask).wait_recv()
    for step in crossing:
        for mask in range(1, depth_count):
            send(step, mask).wait_send()


def local(voxel_bins, colors, opacity, slab_order):
    depth_count = lax.axis_size("depth")
    tile_count = lax.axis_size("screen")
    samples, row_count, cols = voxel_bins.shape
    rows_each = row_count // (depth_count * tile_count)
    unit_rows = max(8, rows_each)
    owners = unit_rows // rows_each
    units = tile_count // owners
    rate = extinction / (samples * depth_count)
    sizes = (depth_count, tile_count, samples, unit_rows, units, owners, rows_each, cols, rate)
    others = depth_count - 1
    return pl.pallas_call(
        functools.partial(kernel, sizes),
        out_shape=pltpu.VMEM((4, rows_each, cols * tile_count), jnp.float32),
        in_specs=[pl.BlockSpec(memory_space=pl.ANY)] * 4,
        out_specs=pl.BlockSpec(memory_space=pltpu.VMEM),
        scratch_shapes=[
            pltpu.SMEM(slab_order.shape[::-1], slab_order.dtype),
            pltpu.VMEM(colors.shape, colors.dtype),
            pltpu.VMEM(opacity.shape, opacity.dtype),
            pltpu.SemaphoreType.DMA((3,)),
            pltpu.VMEM((units, depth_count, samples, unit_rows, cols), jnp.int32),
            pltpu.VMEM((units, others, 4, unit_rows, cols), jnp.float32),
            pltpu.VMEM((units, 4, unit_rows, cols), jnp.float32),
            pltpu.VMEM((units, others, 4, unit_rows, cols), jnp.float32),
            pltpu.VMEM((units, owners, 4, rows_each, cols), jnp.float32),
            pltpu.SemaphoreType.DMA((units, depth_count)),
            pltpu.SemaphoreType.DMA((units, others)),
            pltpu.SemaphoreType.DMA((units, others)),
            pltpu.SemaphoreType.DMA((tile_count,)),
            pltpu.SemaphoreType.DMA((tile_count,)),
            pltpu.SemaphoreType.REGULAR((tile_count,)),
            pltpu.VMEM((depth_count, 4, unit_rows, cols), jnp.float32),
            pltpu.SemaphoreType.DMA((depth_count,)),
            pltpu.SemaphoreType.DMA((depth_count,)),
        ],
        compiler_params=pltpu.CompilerParams(collective_id=0, has_side_effects=True),
    )(slab_order.T, voxel_bins, colors, opacity)


def solution(mesh):
    placed = (P("depth", None, "screen"), P(), P(), P())
    return jax.shard_map(
        local,
        mesh=mesh,
        in_specs=placed,
        out_specs=P(None, ("depth", "screen"), None),
        check_vma=False,
    )
```
